32 devices in a mesh: unit: 1, dp: 16 (over z, y, x), ens: 2 (over core).
Axes of the slice: x: 2, y: 2, z: 4, core: 2. Of those that a mesh axis runs over, the one named last changes fastest.
Arguments:
- samples_in: bfloat16 [4096, 4096], P(('unit', 'dp'), 'ens'), may hold values from -3 to 3, as said below
- second_samples_in: bfloat16 [4096, 4096], P(('unit', 'dp'), 'ens'), may hold values from -3 to 3, as said below
Outputs:
- scaled: float32 [4096, 4096], P('unit', ('ens', 'dp'))
- second_scaled: float32 [4096, 4096], P('unit', ('ens', 'dp'))
The draws below stay inside these ranges and needn't reach their ends.
Inputs may be any that keep to these rules, and one draw needn't show every extreme that they name: samples_in holds numbers from -3 to 3. second_samples_in holds numbers from -3 to 3.
All inputs are finite; a program needn't handle non-finite values.
Results may differ from the reference program's by a relative error of at most 0.00035.
Values may be sent and summed in bfloat16 or wider, within the bound.
A program may use at most 128 MiB of HBM per device.

```python
import jax
import jax.numpy as jnp

ROW_DEV = 256
ROWS = 4096
COLS = 4096
N_DP = 16


def column_values(key, tag):
    keys = jax.random.split(jax.random.fold_in(key, tag), 4)
    level = jax.random.normal(keys[0], (1, 1, COLS), jnp.float32) * 0.4
    spread = jnp.exp(jax.random.uniform(keys[1], (1, 1, COLS), jnp.float32, -0.7, 0.7))
    drift = jax.random.normal(keys[2], (N_DP, 1, COLS), jnp.float32) * 0.5
    noise = jax.random.normal(keys[3], (N_DP, ROW_DEV, COLS), jnp.float32) * 0.36
    return level + spread * (drift + noise)


def draw_samples_in(key, part):
    values = column_values(key, 1)
    return jnp.clip(values, -3.0, 3.0).reshape(ROWS, COLS).astype(jnp.bfloat16)


def draw_second_samples_in(key, part):
    values = column_values(key, 2)
    return jnp.clip(values, -3.0, 3.0).reshape(ROWS, COLS).astype(jnp.bfloat16)


def setup_inputs(seed: int = 0, part: int = 0) -> dict:
    key_list = jax.random.split(jax.random.key(seed), 3)
    own_keys = jax.random.split(jax.random.fold_in(key_list[2], part), 3)
    samples_in = draw_samples_in(jax.random.fold_in(jax.random.fold_in(key_list[2], part), 71), part)
    second_samples_in = draw_second_samples_in(jax.random.fold_in(jax.random.fold_in(key_list[2], part), 71), part)
    return {"samples_in": samples_in, "second_samples_in": second_samples_in}


def reference(samples_in, second_samples_in):
    wide_scaled = samples_in.astype(jnp.float32)
    power_scaled = jnp.exp(wide_scaled)
    sum_scaled = jnp.sum(power_scaled, axis=0)
    scaled = (power_scaled / sum_scaled * ROWS)
    wide_second_scaled = second_samples_in.astype(jnp.float32)
    power_second_scaled = jnp.exp(wide_second_scaled)
    sum_second_scaled = jnp.sum(power_second_scaled, axis=0)
    second_scaled = (power_second_scaled / sum_second_scaled * ROWS)
    return scaled, second_scaled
```

```python
import functools

import jax
import jax.numpy as jnp
from jax import lax
from jax.experimental import pallas as pl
from jax.experimental.pallas import tpu as pltpu
from jax.sharding import PartitionSpec as P

MESH = pl.DeviceIdType.MESH


def send_orders(n):
    quarter = max(n // 4, 1)
    near = list(range(1, quarter))
    side = list(range(quarter, n // 2))
    far = [k for i in range(quarter) for k in (3 * quarter + i, 2 * quarter + i)]
    outer = side + far[:2] + near + far[2:]
    inner = far[:2] + near
    rest, sides = far[2:], list(side)
    while rest or sides:
        inner += rest[:2]
        rest = rest[2:]
        inner += sides[:1]
        sides = sides[1:]
    waits = near + side + far
    return outer, inner, waits


def partner(me, k, n):
    total, bit = 0, 1
    while bit < n:
        total = total + ((me // bit + k // bit) % 2) * bit
        bit *= 2
    return total


def exchange(n, x0, x1, p0, p1, scale, in0, in1, held, load_sem, send_sem, recv_sem):
    xs, ins, ps = (x0, x1), (in0, in1), (p0, p1)
    rows, width = x0.shape[0], x0.shape[1] // n
    me = lax.axis_index("dp")
    outer_order, inner_order, wait_order = send_orders(n)
    quarter_of_me = me * 4 // n
    inner = (quarter_of_me + 1) // 2 % 2

    loads = [pltpu.make_async_copy(xs[a], ins[a], load_sem.at[a]) for a in range(2)]
    for load in loads:
        load.start()

    barrier = pltpu.get_barrier_semaphore()
    for k in range(1, n):
        pl.semaphore_signal(barrier, inc=1, device_id={"dp": partner(me, k, n)}, device_id_type=MESH)
    pl.semaphore_wait(barrier, n - 1)

    for load in loads:
        load.wait()

    def copy(a, k, to, at):
        return pltpu.make_async_remote_copy(
            src_ref=ins[a].at[:, pl.ds(pl.multiple_of(to * width, width), width)],
            dst_ref=held.at[a, pl.ds(pl.multiple_of(at * rows, rows), rows), :],
            send_sem=send_sem.at[a, k],
            recv_sem=recv_sem.at[a, k],
            device_id={"dp": to},
            device_id_type=MESH,
        )

    for from_outer, from_inner in zip(outer_order, inner_order):
        k = from_outer + inner * (from_inner - from_outer)
        to = partner(me, k, n)
        for a in range(2):
            copy(a, k, to, me).start()

    def raised(block):
        power = jnp.exp(block.astype(jnp.float32))
        return power, jnp.sum(power.reshape(rows // 8, 8, width), axis=0)

    own_rows = pl.ds(pl.multiple_of(me * rows, rows), rows)
    own_columns = pl.ds(pl.multiple_of(me * width, width), width)
    sums = []
    for a in range(2):
        power, part = raised(ins[a][:, own_columns])
        ps[a][own_rows, :] = power
        sums.append(part)
    for k in wait_order:
        source = partner(me, k, n)
        its_rows = pl.ds(pl.multiple_of(source * rows, rows), rows)
        for a in range(2):
            copy(a, k, source, source).wait_recv()
            power, part = raised(held[a, its_rows, :])
            ps[a][its_rows, :] = power
            sums[a] = sums[a] + part
    for a in range(2):
        scale[a] = jnp.broadcast_to(n * rows / jnp.sum(sums[a], axis=0, keepdims=True), (8, width))
    for k in wait_order:
        to = partner(me, k, n)
        for a in range(2):
            copy(a, k, to, me).wait_send()


def per_device(n, samples_in, second_samples_in):
    rows, wide = samples_in.shape
    width = wide // n
    in_hbm = pl.BlockSpec(memory_space=pltpu.HBM)
    scratch_bytes = 4 * rows * wide * samples_in.dtype.itemsize
    in_vmem = pl.BlockSpec(memory_space=pltpu.VMEM)
    power_scaled, power_second_scaled, scale = pl.pallas_call(
        functools.partial(exchange, n),
        out_shape=(
            pltpu.VMEM((n * rows, width), jnp.float32),
            pltpu.VMEM((n * rows, width), jnp.float32),
            pltpu.VMEM((2, 8, width), jnp.float32),
        ),
        in_specs=[in_hbm] * 2,
        out_specs=(in_vmem,) * 3,
        scratch_shapes=[
            pltpu.VMEM((rows, wide), samples_in.dtype),
            pltpu.VMEM((rows, wide), samples_in.dtype),
            pltpu.VMEM((2, n * rows, width), samples_in.dtype),
            pltpu.SemaphoreType.DMA((2,)),
            pltpu.SemaphoreType.DMA((2, n)),
            pltpu.SemaphoreType.DMA((2, n)),
        ],
        compiler_params=pltpu.CompilerParams(
            collective_id=0,
            has_side_effects=True,
            vmem_limit_bytes=scratch_bytes + 2**21,
        ),
    )(samples_in, second_samples_in)
    return power_scaled * scale[0, :1], power_second_scaled * scale[1, :1]


def solution(mesh):
    placed = (P(("unit", "dp"), "ens"), P(("unit", "dp"), "ens"))
    return jax.shard_map(
        functools.partial(per_device, mesh.shape["dp"]),
        mesh=mesh,
        in_specs=placed,
        out_specs=(P("unit", ("ens", "dp")), P("unit", ("ens", "dp"))),
        check_vma=False,
    )
```

```python
import functools

import jax
import jax.numpy as jnp
from jax import lax
from jax.experimental import pallas as pl
from jax.experimental.pallas import tpu as pltpu
from jax.sharding import PartitionSpec as P

MESH = pl.DeviceIdType.MESH


def send_orders(n):
    quarter = max(n // 4, 1)
    near = list(range(1, quarter))
    side = list(range(quarter, n // 2))
    far = [k for i in range(quarter) for k in (3 * quarter + i, 2 * quarter + i)]
    outer = side + far[:2] + near + far[2:]
    inner = far[:2] + near
    rest, sides = far[2:], list(side)
    while rest or sides:
        inner += rest[:2]
        rest = rest[2:]
        inner += sides[:1]
        sides = sides[1:]
    waits = near + side + far
    return outer, inner, waits


def partner(me, k, n):
    total, bit = 0, 1
    while bit < n:
        total = total + ((me // bit + k // bit) % 2) * bit
        bit *= 2
    return total


def exchange(n, x0, x1, p0, p1, scale, in0, in1, held, load_sem, send_sem, recv_sem):
    xs, ins, ps = (x0, x1), (in0, in1), (p0, p1)
    rows, width = x0.shape[0], x0.shape[1] // n
    me = lax.axis_index("dp")
    outer_order, inner_order, wait_order = send_orders(n)
    quarter_of_me = me * 4 // n
    inner = (quarter_of_me + 1) // 2 % 2

    loads = [pltpu.make_async_copy(xs[a], ins[a], load_sem.at[a]) for a in range(2)]
    for load in loads:
        load.start()

    barrier = pltpu.get_barrier_semaphore()
    for k in range(1, n):
        pl.semaphore_signal(barrier, inc=1, device_id={"dp": partner(me, k, n)}, device_id_type=MESH)
    pl.semaphore_wait(barrier, n - 1)

    for load in loads:
        load.wait()

    def copy(a, k, to, at):
        return pltpu.make_async_remote_copy(
            src_ref=ins[a].at[:, pl.ds(pl.multiple_of(to * width, width), width)],
            dst_ref=held.at[a, pl.ds(pl.multiple_of(at * rows, rows), rows), :],
            send_sem=send_sem.at[a, k],
            recv_sem=recv_sem.at[a, k],
            device_id={"dp": to},
            device_id_type=MESH,
        )

    for from_outer, from_inner in zip(outer_order, inner_order):
        k = from_outer + inner * (from_inner - from_outer)
        to = partner(me, k, n)
        for a in range(2):
            copy(a, k, to, me).start()

    def raised(block):
        power = jnp.exp(block.astype(jnp.float32))
        return power, jnp.sum(power.reshape(rows // 8, 8, width), axis=0)

    own_rows = pl.ds(pl.multiple_of(me * rows, rows), rows)
    own_columns = pl.ds(pl.multiple_of(me * width, width), width)
    sums = []
    for a in range(2):
        power, part = raised(ins[a][:, own_columns])
        ps[a][own_rows, :] = power
        sums.append(part)
    for k in wait_order:
        source = partner(me, k, n)
        its_rows = pl.ds(pl.multiple_of(source * rows, rows), rows)
        for a in range(2):
            copy(a, k, source, source).wait_recv()
            power, part = raised(held[a, its_rows, :])
            ps[a][its_rows, :] = power
            sums[a] = sums[a] + part
    for a in range(2):
        scale[a] = jnp.broadcast_to(n * rows / jnp.sum(sums[a], axis=0, keepdims=True), (8, width))
    for k in wait_order:
        to = partner(me, k, n)
        for a in range(2):
            copy(a, k, to, me).wait_send()


def per_device(n, samples_in, second_samples_in):
    rows, wide = samples_in.shape
    width = wide // n
    in_hbm = pl.BlockSpec(memory_space=pltpu.HBM)
    out_bytes = 2 * n * rows * width * 4
    in_vmem = pl.BlockSpec(memory_space=pltpu.VMEM)
    power_scaled, power_second_scaled, scale = pl.pallas_call(
        functools.partial(exchange, n),
        out_shape=(
            pltpu.VMEM((n * rows, width), jnp.float32),
            pltpu.VMEM((n * rows, width), jnp.float32),
            pltpu.VMEM((2, 8, width), jnp.float32),
        ),
        in_specs=[in_hbm] * 2,
        out_specs=(in_vmem,) * 3,
        scratch_shapes=[
            pltpu.VMEM((rows, wide), samples_in.dtype),
            pltpu.VMEM((rows, wide), samples_in.dtype),
            pltpu.VMEM((2, n * rows, width), samples_in.dtype),
            pltpu.SemaphoreType.DMA((2,)),
            pltpu.SemaphoreType.DMA((2, n)),
            pltpu.SemaphoreType.DMA((2, n)),
        ],
        compiler_params=pltpu.CompilerParams(
            collective_id=0,
            has_side_effects=True,
            vmem_limit_bytes=67043328 - out_bytes - 2**19,
        ),
    )(samples_in, second_samples_in)
    return power_scaled * scale[0, :1], power_second_scaled * scale[1, :1]


def solution(mesh):
    placed = (P(("unit", "dp"), "ens"), P(("unit", "dp"), "ens"))
    return jax.shard_map(
        functools.partial(per_device, mesh.shape["dp"]),
        mesh=mesh,
        in_specs=placed,
        out_specs=(P("unit", ("ens", "dp")), P("unit", ("ens", "dp"))),
        check_vma=False,
    )
```

```python
import functools

import jax
import jax.numpy as jnp
from jax import lax
from jax.experimental import pallas as pl
from jax.experimental.pallas import tpu as pltpu
from jax.sharding import PartitionSpec as P

MESH = pl.DeviceIdType.MESH


def send_orders(n):
    quarter = max(n // 4, 1)
    near = list(range(1, quarter))
    side = list(range(quarter, n // 2))
    to_own_kind = list(range(3 * quarter, n))
    to_other_kind = list(range(2 * quarter, 3 * quarter))

    def far_first_to_outer(outer_bound, inner_bound):
        half = (quarter + 1) // 2
        far = [k for pair in zip(outer_bound, inner_bound) for k in pair][: 2 * half]
        return far + outer_bound[half:] + inner_bound[half:]

    far = far_first_to_outer(to_own_kind, to_other_kind)
    outer = side + far[:2] + near + far[2:]
    rest = far_first_to_outer(to_other_kind, to_own_kind)
    inner, rest = rest[:2] + near, rest[2:]
    for i in range(max(len(rest), len(side))):
        inner += side[i : i + 1] + rest[i : i + 1]
    waits = near + side + far
    return outer, inner, waits


def partner(me, k, n):
    total, bit = 0, 1
    while bit < n:
        total = total + ((me // bit + k // bit) % 2) * bit
        bit *= 2
    return total


def exchange(n, x0, x1, p0, p1, scale, in0, in1, held, load_sem, send_sem, recv_sem):
    xs, ins, ps = (x0, x1), (in0, in1), (p0, p1)
    rows, width = x0.shape[0], x0.shape[1] // n
    me = lax.axis_index("dp")
    outer_order, inner_order, wait_order = send_orders(n)
    quarter_of_me = me * 4 // n
    inner = (quarter_of_me + 1) // 2 % 2

    loads = [pltpu.make_async_copy(xs[a], ins[a], load_sem.at[a]) for a in range(2)]
    for load in loads:
        load.start()

    barrier = pltpu.get_barrier_semaphore()
    for k in range(1, n):
        pl.semaphore_signal(barrier, inc=1, device_id={"dp": partner(me, k, n)}, device_id_type=MESH)
    pl.semaphore_wait(barrier, n - 1)

    for load in loads:
        load.wait()

    def copy(a, k, to, at):
        return pltpu.make_async_remote_copy(
            src_ref=ins[a].at[:, pl.ds(pl.multiple_of(to * width, width), width)],
            dst_ref=held.at[a, pl.ds(pl.multiple_of(at * rows, rows), rows), :],
            send_sem=send_sem.at[a, k],
            recv_sem=recv_sem.at[a, k],
            device_id={"dp": to},
            device_id_type=MESH,
        )

    for from_outer, from_inner in zip(outer_order, inner_order):
        k = from_outer + inner * (from_inner - from_outer)
        to = partner(me, k, n)
        for a in range(2):
            copy(a, k, to, me).start()

    def raised(block):
        power = jnp.exp(block.astype(jnp.float32))
        return power, jnp.sum(power.reshape(rows // 8, 8, width), axis=0)

    own_rows = pl.ds(pl.multiple_of(me * rows, rows), rows)
    own_columns = pl.ds(pl.multiple_of(me * width, width), width)
    sums = []
    for a in range(2):
        power, part = raised(ins[a][:, own_columns])
        ps[a][own_rows, :] = power
        sums.append(part)
    for k in wait_order:
        source = partner(me, k, n)
        its_rows = pl.ds(pl.multiple_of(source * rows, rows), rows)
        for a in range(2):
            copy(a, k, source, source).wait_recv()
            power, part = raised(held[a, its_rows, :])
            ps[a][its_rows, :] = power
            sums[a] = sums[a] + part
    for a in range(2):
        scale[a] = jnp.broadcast_to(n * rows / jnp.sum(sums[a], axis=0, keepdims=True), (8, width))
    for k in wait_order:
        to = partner(me, k, n)
        for a in range(2):
            copy(a, k, to, me).wait_send()


def per_device(n, samples_in, second_samples_in):
    rows, wide = samples_in.shape
    width = wide // n
    in_hbm = pl.BlockSpec(memory_space=pltpu.HBM)
    out_bytes = 2 * n * rows * width * 4
    in_vmem = pl.BlockSpec(memory_space=pltpu.VMEM)
    power_scaled, power_second_scaled, scale = pl.pallas_call(
        functools.partial(exchange, n),
        out_shape=(
            pltpu.VMEM((n * rows, width), jnp.float32),
            pltpu.VMEM((n * rows, width), jnp.float32),
            pltpu.VMEM((2, 8, width), jnp.float32),
        ),
        in_specs=[in_hbm] * 2,
        out_specs=(in_vmem,) * 3,
        scratch_shapes=[
            pltpu.VMEM((rows, wide), samples_in.dtype),
            pltpu.VMEM((rows, wide), samples_in.dtype),
            pltpu.VMEM((2, n * rows, width), samples_in.dtype),
            pltpu.SemaphoreType.DMA((2,)),
            pltpu.SemaphoreType.DMA((2, n)),
            pltpu.SemaphoreType.DMA((2, n)),
        ],
        compiler_params=pltpu.CompilerParams(
            collective_id=0,
            has_side_effects=True,
            vmem_limit_bytes=67043328 - out_bytes - 2**19,
        ),
    )(samples_in, second_samples_in)
    return power_scaled * scale[0, :1], power_second_scaled * scale[1, :1]


def solution(mesh):
    placed = (P(("unit", "dp"), "ens"), P(("unit", "dp"), "ens"))
    return jax.shard_map(
        functools.partial(per_device, mesh.shape["dp"]),
        mesh=mesh,
        in_specs=placed,
        out_specs=(P("unit", ("ens", "dp")), P("unit", ("ens", "dp"))),
        check_vma=False,
    )
```

```python
import functools

import jax
import jax.numpy as jnp
from jax import lax
from jax.experimental import pallas as pl
from jax.experimental.pallas import tpu as pltpu
from jax.sharding import PartitionSpec as P

MESH = pl.DeviceIdType.MESH


def send_orders(n):
    quarter = max(n // 4, 1)
    near = list(range(1, quarter))
    side = list(range(quarter, n // 2))
    to_own_kind = list(range(3 * quarter, n))
    to_other_kind = list(range(2 * quarter, 3 * quarter))

    def far_first_to_outer(outer_bound, inner_bound):
        return [k for pair in zip(outer_bound, inner_bound) for k in pair]

    far = far_first_to_outer(to_own_kind, to_other_kind)
    outer = side + far[:2] + near + far[2:]
    rest = far_first_to_outer(to_other_kind, to_own_kind)
    inner, rest = rest[:2] + near, rest[2:]
    for i in range(max(len(rest), len(side))):
        inner += side[i : i + 1] + rest[i : i + 1]
    waits = near + side + far
    return outer, inner, waits


def partner(me, k, n):
    total, bit = 0, 1
    while bit < n:
        total = total + ((me // bit + k // bit) % 2) * bit
        bit *= 2
    return total


def exchange(n, x0, x1, p0, p1, scale, in0, in1, held, load_sem, send_sem, recv_sem):
    xs, ins, ps = (x0, x1), (in0, in1), (p0, p1)
    rows, width = x0.shape[0], x0.shape[1] // n
    me = lax.axis_index("dp")
    outer_order, inner_order, wait_order = send_orders(n)
    quarter_of_me = me * 4 // n
    inner = (quarter_of_me + 1) // 2 % 2

    loads = [pltpu.make_async_copy(xs[a], ins[a], load_sem.at[a]) for a in range(2)]
    for load in loads:
        load.start()

    barrier = pltpu.get_barrier_semaphore()
    for k in range(1, n):
        pl.semaphore_signal(barrier, inc=1, device_id={"dp": partner(me, k, n)}, device_id_type=MESH)
    pl.semaphore_wait(barrier, n - 1)

    for load in loads:
        load.wait()

    def copy(a, k, to, at):
        return pltpu.make_async_remote_copy(
            src_ref=ins[a].at[:, pl.ds(pl.multiple_of(to * width, width), width)],
            dst_ref=held.at[a, pl.ds(pl.multiple_of(at * rows, rows), rows), :],
            send_sem=send_sem.at[a, k],
            recv_sem=recv_sem.at[a, k],
            device_id={"dp": to},
            device_id_type=MESH,
        )

    for from_outer, from_inner in zip(outer_order, inner_order):
        k = from_outer + inner * (from_inner - from_outer)
        to = partner(me, k, n)
        for a in range(2):
            copy(a, k, to, me).start()

    def raised(block):
        power = jnp.exp(block.astype(jnp.float32))
        return power, jnp.sum(power.reshape(rows // 8, 8, width), axis=0)

    own_rows = pl.ds(pl.multiple_of(me * rows, rows), rows)
    own_columns = pl.ds(pl.multiple_of(me * width, width), width)
    sums = []
    for a in range(2):
        power, part = raised(ins[a][:, own_columns])
        ps[a][own_rows, :] = power
        sums.append(part)
    for k in wait_order:
        source = partner(me, k, n)
        its_rows = pl.ds(pl.multiple_of(source * rows, rows), rows)
        for a in range(2):
            copy(a, k, source, source).wait_recv()
            power, part = raised(held[a, its_rows, :])
            ps[a][its_rows, :] = power
            sums[a] = sums[a] + part
    for a in range(2):
        scale[a] = jnp.broadcast_to(n * rows / jnp.sum(sums[a], axis=0, keepdims=True), (8, width))
    for k in wait_order:
        to = partner(me, k, n)
        for a in range(2):
            copy(a, k, to, me).wait_send()


def per_device(n, samples_in, second_samples_in):
    rows, wide = samples_in.shape
    width = wide // n
    in_hbm = pl.BlockSpec(memory_space=pltpu.HBM)
    out_bytes = 2 * n * rows * width * 4
    in_vmem = pl.BlockSpec(memory_space=pltpu.VMEM)
    power_scaled, power_second_scaled, scale = pl.pallas_call(
        functools.partial(exchange, n),
        out_shape=(
            pltpu.VMEM((n * rows, width), jnp.float32),
            pltpu.VMEM((n * rows, width), jnp.float32),
            pltpu.VMEM((2, 8, width), jnp.float32),
        ),
        in_specs=[in_hbm] * 2,
        out_specs=(in_vmem,) * 3,
        scratch_shapes=[
            pltpu.VMEM((rows, wide), samples_in.dtype),
            pltpu.VMEM((rows, wide), samples_in.dtype),
            pltpu.VMEM((2, n * rows, width), samples_in.dtype),
            pltpu.SemaphoreType.DMA((2,)),
            pltpu.SemaphoreType.DMA((2, n)),
            pltpu.SemaphoreType.DMA((2, n)),
        ],
        compiler_params=pltpu.CompilerParams(
            collective_id=0,
            has_side_effects=True,
            vmem_limit_bytes=67043328 - out_bytes - 2**19,
        ),
    )(samples_in, second_samples_in)
    return power_scaled * scale[0, :1], power_second_scaled * scale[1, :1]


def solution(mesh):
    placed = (P(("unit", "dp"), "ens"), P(("unit", "dp"), "ens"))
    return jax.shard_map(
        functools.partial(per_device, mesh.shape["dp"]),
        mesh=mesh,
        in_specs=placed,
        out_specs=(P("unit", ("ens", "dp")), P("unit", ("ens", "dp"))),
        check_vma=False,
    )
```
